32 devices in a mesh: grp: 2 (over x), ha: 16 (over z, y, core).
Axes of the slice: x: 2, y: 2, z: 4, core: 2. Of those that a mesh axis runs over, the one named last changes fastest.
Arguments:
- tokens: bfloat16 [8192, 5120], P(('grp', 'ha')), parts along dimension 0, may hold values from -6 to 6
- mod_shift: float32 [10240], P('grp'), parts along dimension 0, may hold values from -4 to 4
- mod_scale: float32 [10240], P('grp'), parts along dimension 0, may hold values from 0.25 to 1.75
- head_weight: bfloat16 [5120, 64], replicated, may hold values from -0.078125 to 0.078125
- head_bias: float32 [64], replicated, may hold values from -3 to 3
- first_kernel: bfloat16 [3, 3, 3, 16, 384], replicated, may hold values from -0.3125 to 0.3125
- first_bias: float32 [384], replicated, may hold values from -3 to 3
- norm_gain: float32 [384], replicated, may hold values from 0.25 to 1.75
- second_kernel: bfloat16 [3, 3, 3, 384, 384], replicated, may hold values from -0.0625 to 0.0625
- second_bias: float32 [384], replicated, may hold values from -2 to 2
Outputs:
- decoded: bfloat16 [4, 64, 128, 384], P(None, ('grp', 'ha')), parts along dimension 1
The draws below stay inside these ranges and needn't reach their ends.
There are 2 independent parts, one for each index of `grp`. The reference program is written for one: setup_inputs(seed, part) draws one part's arguments, and reference() takes and returns one part's arrays. A program takes and returns all parts, laid end to end along the dimension named above; an argument that names none is the same for every part. Nothing has to cross between parts.
All inputs are finite; a program needn't handle non-finite values.
Results may differ from the reference program's by a relative error of at most 0.0059.
Values may be sent and summed in bfloat16 or wider, within the bound.
A program may use at most 64 MiB of HBM per device.

```python
import jax
import jax.numpy as jnp
from jax import lax

D = 5120
LAT_CH = 16
CH = 384
FRAMES = 4
HB = 2
W = 128
HEAD_OUT = 64
TOKENS = 4096
N_HA = 16


def block_scale(own_key, dims, shards, smallest, high):
    level, own = 1.0, jax.random.fold_in(own_key, 6)
    for dim, shards_of in shards:
        steps = jnp.exp(jax.random.uniform(jax.random.fold_in(own, dim), (shards_of,), jnp.float32, smallest / len(shards), high / len(shards)))
        level = level * jnp.repeat(steps, dims[dim] // shards_of).reshape([-1 if axis == dim else 1 for axis in range(len(dims))])
    return level


def noise(own_key, shape, scale, bound, split=(), kind=jnp.bfloat16):
    entries = jax.random.normal(own_key, shape, jnp.float32) * scale
    if len(split) > 0:
        entries = block_scale(own_key, shape, split, -0.22, 0.18) * entries
    return jnp.clip(entries, min=-bound, max=bound).astype(kind)


def setup_inputs(seed: int = 0, part: int = 0) -> dict:
    streams_of = jax.random.split(jax.random.key(seed), 11)
    own_keys = jax.random.split(jax.random.fold_in(streams_of[10], part), 11)
    return {
        "tokens": noise(own_keys[0], (TOKENS, D), 1.0, 6.0, ((0, 16),)),
        "mod_shift": noise(own_keys[1], (D,), 1.0, 4.0, (), jnp.float32),
        "mod_scale": jnp.clip(1.0 + 0.15 * jax.random.normal(own_keys[2], (D,), jnp.float32), 0.25, 1.75),
        "head_weight": noise(streams_of[3], (D, HEAD_OUT), D ** -0.5, 0.078125),
        "head_bias": noise(streams_of[4], (HEAD_OUT,), 0.5, 3.0, (), jnp.float32),
        "first_kernel": noise(streams_of[5], (3, 3, 3, LAT_CH, CH), (27 * LAT_CH) ** -0.5, 0.3125),
        "first_bias": noise(streams_of[6], (CH,), 0.5, 3.0, (), jnp.float32),
        "norm_gain": jnp.clip(1.0 + 0.15 * jax.random.normal(streams_of[7], (CH,), jnp.float32), 0.25, 1.75),
        "second_kernel": noise(streams_of[8], (3, 3, 3, CH, CH), (27 * CH) ** -0.5, 0.0625),
        "second_bias": noise(streams_of[9], (CH,), 0.3, 2.0, (), jnp.float32),
    }


def output_head(tokens, mod_shift, mod_scale, head_weight, head_bias):
    values = tokens.astype(jnp.float32)
    centred = values - lax.optimization_barrier(jnp.mean(values, axis=-1, keepdims=True))
    spread = lax.optimization_barrier(jnp.mean(centred * centred, axis=-1, keepdims=True))
    normed = centred * lax.rsqrt(spread + 1e-06)
    modulated = (normed * mod_scale + mod_shift).astype(jnp.bfloat16)
    result = jnp.dot(modulated, head_weight, preferred_element_type=jnp.float32) + head_bias
    return result.astype(jnp.bfloat16)

def unpatch(rows, frames, prows, pcols):
    shaped = rows.reshape(frames, prows, pcols, 2, 2, LAT_CH)
    shaped = shaped.transpose(0, 1, 3, 2, 4, 5)
    return shaped.reshape(frames, 2 * prows, 2 * pcols, LAT_CH)

def causal_conv(field, kernel, bias):
    padded = jnp.pad(field.astype(jnp.float32), ((2, 0), (0, 0), (1, 1), (0, 0)))
    result = lax.conv_general_dilated(padded[None], kernel.astype(jnp.float32), (1, 1, 1), 'VALID', dimension_numbers=('NDHWC', 'DHWIO', 'NDHWC'), precision=lax.Precision.HIGHEST, preferred_element_type=jnp.float32)[0]
    return result + bias

def activate(field, gain):
    meansq = lax.optimization_barrier(jnp.mean(field * field, axis=-1, keepdims=True))
    return jax.nn.silu(field * lax.rsqrt(meansq + 1e-06) * gain).astype(jnp.bfloat16)

def reference(tokens, mod_shift, mod_scale, head_weight, head_bias, first_kernel, first_bias, norm_gain, second_kernel, second_bias):
    head = output_head(tokens, mod_shift, mod_scale, head_weight, head_bias)
    latent = unpatch(head, FRAMES, HB * N_HA // 2, W // 2)
    widened = jnp.pad(latent, ((0, 0), (1, 1), (0, 0), (0, 0)))
    first = causal_conv(widened, first_kernel, first_bias)
    hidden = activate(first, norm_gain)
    beside_all = jnp.pad(hidden, ((0, 0), (1, 1), (0, 0), (0, 0)))
    second = causal_conv(beside_all, second_kernel, second_bias)
    return second.astype(jnp.bfloat16)
```

```python
import functools

import jax
import jax.numpy as jnp
from jax import lax
from jax.experimental import pallas as pl
from jax.experimental.pallas import tpu as pltpu
from jax.sharding import PartitionSpec as P

FRAMES = 4
VMEM_BYTES = 56_000_000
GROUP = 2
MESH = pl.DeviceIdType.MESH
F32, BF16 = jnp.float32, jnp.bfloat16


def iota(shape, dim):
    return lax.broadcasted_iota(jnp.int32, shape, dim)


def expansion(lch):
    wide = 4 * lch
    i = iota((2 * wide, 6 * 2 * wide), 0)
    o = iota((2 * wide, 6 * 2 * wide), 1)
    half, q, r, k = i // wide, i // (2 * lch) % 2, i // lch % 2, i % lch
    block, lane = o // (2 * wide), o % (2 * wide)
    ohalf, kind = block // 3, block % 3
    oq, j, ok = lane // wide, lane // lch % 4, lane % lch
    same = (half == ohalf) & (q == oq) & (k == ok)
    own = (kind == 0) & (j == r + 1)
    before = (kind == 1) & (r == 1) & (j == 0)
    after = (kind == 2) & (r == 0) & (j == 3)
    return jnp.where(same & (own | before | after), 1.0, 0.0).astype(BF16)


def kernel(
    n, lch, ch,
    tokens, shift_in, scale_in, hw, hbias_in, k1, b1_in, gain_in, k2, b2_in, obuf,
    tok, hwv, k1v, w1, w2, send, recv, patches, hid, z, inter,
    shift, scale, hbias, b1, gain, b2,
    tok_sem, hw_sem, k1_sem, w2_sem, send_sem, recv_sem, small_sem,
):
    me = lax.axis_index("ha")
    per = n // FRAMES
    mine = lax.rem(me, per) * FRAMES
    frame = lax.div(me, per)
    cells = tok.shape[0] // FRAMES
    half = cells // 2
    width = tok.shape[1]
    wide = 4 * lch
    lanes = 2 * wide

    step = GROUP * cells
    steps = FRAMES // GROUP
    def token_copies(g):
        for i in range(g * GROUP, (g + 1) * GROUP):
            rows = pl.ds(i * cells, cells)
            yield pltpu.make_async_copy(tokens.at[rows], tok.at[rows], tok_sem.at[i])

    small = [
        pltpu.make_async_copy(src, dst, small_sem.at[i])
        for i, (src, dst) in enumerate(zip((scale_in, shift_in, hbias_in, b1_in, gain_in, b2_in), (scale, shift, hbias, b1, gain, b2)))
    ]
    for copy in token_copies(0):
        copy.start()
    for g in range(2):
        pltpu.make_async_copy(hw, hwv.at[pl.ds(g * wide, wide)], hw_sem.at[g]).start()
    for copy in small:
        copy.start()

    barrier = pltpu.get_barrier_semaphore()
    for f in range(FRAMES):
        for g in range(3):
            p = me + g - 1
            src = f * per + lax.div(jnp.clip(p, 0, n - 1), FRAMES)

            @pl.when((p >= 0) & (p < n) & (src != me))
            def _():
                pl.semaphore_signal(barrier, inc=1, device_id={"ha": src}, device_id_type=MESH)

    def targets(j):
        for g in range(3):
            to = mine + j + 1 - g
            yield g, to, (to >= 0) & (to < n)

    credits = 0
    for j in range(FRAMES):
        for g, to, ok in targets(j):
            credits = credits + jnp.where(ok & (to != me), 1, 0)

    w1[...] = jnp.zeros_like(w1)
    for g in (0, 2):
        @pl.when(me == (0 if g == 0 else n - 1))
        def _():
            for f in range(FRAMES):
                recv[f, g] = jnp.zeros((half, lanes), BF16)

    def head_rows(s):
        rows = pl.ds(s * step, step)
        acc = jnp.zeros((step, 128), F32)
        for c in range(0, width, 128):
            acc += tok[rows, c:c + 128].astype(F32)
        mean = jnp.sum(acc, axis=1, keepdims=True) * (1.0 / width)
        acc = jnp.zeros((step, 128), F32)
        for c in range(0, width, 128):
            centred = tok[rows, c:c + 128].astype(F32) - mean
            acc += centred * centred
        spread = jnp.sum(acc, axis=1, keepdims=True) * (1.0 / width)
        inv = lax.rsqrt(spread + 1e-06)
        if s == 0:
            for g in range(2):
                pltpu.make_async_copy(hw, hwv.at[pl.ds(g * wide, wide)], hw_sem.at[g]).wait()
            for copy in small:
                copy.wait()
        total = jnp.zeros((step, lanes), F32)
        for c in range(0, width, 512):
            centred = tok[rows, c:c + 512].astype(F32) - mean
            modulated = (centred * inv * scale[:, c:c + 512] + shift[:, c:c + 512]).astype(BF16)
            total += lax.dot_general(modulated, hwv[:, c:c + 512], (((1,), (1,)), ((), ())), preferred_element_type=F32)
        total = total + jnp.concatenate([hbias[...], hbias[...]], axis=1)
        low = iota((half, lanes), 1) < wide
        for a in range(GROUP):
            row = total[a * cells:(a + 1) * cells]
            send[s * GROUP + a] = jnp.where(low, row[:half], row[half:]).astype(BF16)

    for s in range(steps):
        for copy in token_copies(s):
            copy.wait()
        if s + 1 < steps:
            for copy in token_copies(s + 1):
                copy.start()
        if s == 0:
            pltpu.make_async_copy(k1, k1v, k1_sem).start()
        if s == steps - 1:
            for t in range(9):
                for dx in range(3):
                    pltpu.make_async_copy(k2.at[t * 3 + dx], w2.at[pl.ds(t * ch, ch), pl.ds(dx * ch, ch)], w2_sem.at[t * 3 + dx]).start()
        head_rows(s)
        if s == 0:
            pl.semaphore_wait(barrier, credits)
        for a in range(GROUP):
            j = s * GROUP + a
            for g, to, ok in targets(j):
                @pl.when(ok & (to != me))
                def _():
                    pltpu.make_async_remote_copy(
                        src_ref=send.at[j], dst_ref=recv.at[frame, g],
                        send_sem=send_sem.at[j, g], recv_sem=recv_sem.at[frame, g],
                        device_id={"ha": to}, device_id_type=MESH,
                    ).start()

                @pl.when(ok & (to == me))
                def _():
                    pltpu.make_async_copy(send.at[j], recv.at[frame, g], recv_sem.at[frame, g]).start()

    pltpu.make_async_copy(k1, k1v, k1_sem).wait()
    tap = 3 * lch
    for dt in range(3):
        for s in range(2):
            for r in range(2):
                for dy in range(3):
                    top = dt * 2 * lanes + (dy + s) * wide + r * lch
                    w1[top:top + tap, (2 * s + r) * ch:(2 * s + r + 1) * ch] = k1v[(dt * 3 + dy) * tap:(dt * 3 + dy + 1) * tap, :]
    spread_lanes = expansion(lch)
    place = iota((cells, lanes), 0)
    bias1, gains = [jnp.concatenate([v[i:i + 1] for i in range(ch // 128)], axis=1) for v in (b1, gain)]

    for t in range(9):
        for dx in range(3):
            pltpu.make_async_copy(k2.at[t * 3 + dx], w2.at[pl.ds(t * ch, ch), pl.ds(dx * ch, ch)], w2_sem.at[t * 3 + dx]).wait()

    edge = iota((cells, 128), 0)
    for g in range(3):
        @pl.when((me + g - 1 >= 0) & (me + g - 1 < n))
        def _():
            for f in range(FRAMES):
                pltpu.make_async_copy(send.at[0], recv.at[f, g], recv_sem.at[f, g]).wait()

    def hidden_frame(f):
        rows = recv[f].reshape(3 * half, lanes)
        opened = jnp.dot(rows, spread_lanes, preferred_element_type=F32)
        for g in range(3):
            got = opened[g * half:(g + 1) * half]
            own, before, after = [
                jnp.concatenate([got[:, kind * lanes:(kind + 1) * lanes], got[:, (3 + kind) * lanes:(4 + kind) * lanes]], axis=0)
                for kind in range(3)
            ]
            before = jnp.where(place == 0, 0.0, pltpu.roll(before, 1, 0))
            after = jnp.where(place == cells - 1, 0.0, pltpu.roll(after, cells - 1, 0))
            patches[f, :, g * lanes:(g + 1) * lanes] = (own + before + after).astype(BF16)

        first_dt = max(0, 2 - f)
        for pair in range(2):
            left = jnp.concatenate(
                [patches[f + dt - 2, :, pair * lanes:(pair + 2) * lanes] for dt in range(first_dt, 3)], axis=1)
            for s in range(2):
                y = 2 * pair + s
                first = jnp.dot(left, w1[first_dt * 2 * lanes:, 2 * s * ch:2 * (s + 1) * ch], preferred_element_type=F32)
                for r in range(2):
                    v = first[:, r * ch:(r + 1) * ch] + bias1
                    meansq = jnp.sum(v * v, axis=1, keepdims=True) * (1.0 / ch)
                    v = v * lax.rsqrt(meansq + 1e-06) * gains
                    v = 0.5 * v
                    v = v * jnp.tanh(v) + v
                    if y == 0:
                        v = jnp.where(me == 0, 0.0, v)
                    if y == 3:
                        v = jnp.where(me == n - 1, 0.0, v)
                    hid[f, y, r * cells:(r + 1) * cells, :] = v.astype(BF16)

    def decoded_frame(f):
        first_dt = max(0, 2 - f)
        left = jnp.concatenate(
            [hid[f + dt - 2, dy:dy + 2].reshape(4 * cells, ch) for dt in range(first_dt, 3) for dy in range(3)], axis=1)
        for c in range(0, 3 * ch, 256):
            e = min(c + 256, 3 * ch)
            z[f, :, c:e] = jnp.dot(left, w2[first_dt * 3 * ch:, c:e], preferred_element_type=F32)
        for y in range(2):
            def part(r, dx, c):
                top = (2 * y + r) * cells
                return z[f, top:top + cells, dx * ch + c:dx * ch + c + 128]

            for c in range(0, ch, 128):
                bias = b2[c // 128:c // 128 + 1]
                before = jnp.where(edge == 0, 0.0, pltpu.roll(part(1, 0, c), 1, 0))
                after = jnp.where(edge == cells - 1, 0.0, pltpu.roll(part(0, 2, c), cells - 1, 0))
                lane = inter.at[f, y, c // 128]
                lane[pl.ds(0, cells, stride=2), :] = before + part(0, 1, c) + part(1, 2, c) + bias
                lane[pl.ds(1, cells, stride=2), :] = part(0, 0, c) + part(1, 1, c) + after + bias
                obuf[f, y, :, c:c + 128] = lane[...].astype(BF16)

    hidden_frame(0)
    for f in range(FRAMES):
        if f + 1 < FRAMES:
            hidden_frame(f + 1)
        decoded_frame(f)

    for j in range(FRAMES):
        for g, to, ok in targets(j):
            @pl.when(ok & (to != me))
            def _():
                pltpu.make_async_remote_copy(
                    src_ref=send.at[j], dst_ref=recv.at[frame, g],
                    send_sem=send_sem.at[j, g], recv_sem=recv_sem.at[frame, g],
                    device_id={"ha": to}, device_id_type=MESH,
                ).wait_send()


def store_kernel(held, out, sem):
    copies = [pltpu.make_async_copy(held.at[f], out.at[f], sem.at[f]) for f in range(FRAMES)]
    for copy in copies:
        copy.start()
    for copy in copies:
        copy.wait()


def on_device(tokens, mod_shift, mod_scale, head_weight, head_bias, first_kernel, first_bias, norm_gain, second_kernel, second_bias):
    n = lax.axis_size("ha")
    count, width = tokens.shape
    lch, ch = first_kernel.shape[3:]
    cells = count // FRAMES
    lanes = 8 * lch
    anywhere = pl.BlockSpec(memory_space=pl.ANY)
    vmem = pl.BlockSpec(memory_space=pltpu.VMEM)
    dma = pltpu.SemaphoreType.DMA
    held = pl.pallas_call(
        functools.partial(kernel, n, lch, ch),
        name="decode",
        out_shape=pltpu.VMEM((FRAMES, 2, 2 * cells, ch), BF16),
        in_specs=[anywhere] * 10,
        out_specs=vmem,
        scratch_shapes=[
            pltpu.VMEM((count, width), BF16),
            pltpu.VMEM((lanes, width), BF16),
            pltpu.VMEM((27 * lch, ch), BF16),
            pltpu.VMEM((6 * lanes, 4 * ch), BF16),
            pltpu.VMEM((9 * ch, 3 * ch), BF16),
            pltpu.VMEM((FRAMES, cells // 2, lanes), BF16),
            pltpu.VMEM((FRAMES, 3, cells // 2, lanes), BF16),
            pltpu.VMEM((FRAMES, cells, 3 * lanes), BF16),
            pltpu.VMEM((FRAMES, 4, 2 * cells, ch), BF16),
            pltpu.VMEM((FRAMES, 4 * cells, 3 * ch), F32),
            pltpu.VMEM((FRAMES, 2, ch // 128, 2 * cells, 128), F32),
            pltpu.VMEM((1, width), F32),
            pltpu.VMEM((1, width), F32),
            pltpu.VMEM((1, 4 * lch), F32),
            pltpu.VMEM((ch // 128, 128), F32),
            pltpu.VMEM((ch // 128, 128), F32),
            pltpu.VMEM((ch // 128, 128), F32),
            dma((FRAMES,)),
            dma((2,)),
            dma,
            dma((27,)),
            dma((FRAMES, 3)),
            dma((FRAMES, 3)),
            dma((6,)),
        ],
        compiler_params=pltpu.CompilerParams(collective_id=0, has_side_effects=True, vmem_limit_bytes=VMEM_BYTES),
    )(
        tokens, mod_shift.reshape(1, width), mod_scale.reshape(1, width), head_weight.T, head_bias.reshape(1, -1),
        first_kernel.reshape(27 * lch, ch), first_bias.reshape(-1, 128), norm_gain.reshape(-1, 128),
        second_kernel.reshape(27, ch, ch), second_bias.reshape(-1, 128),
    )
    return pl.pallas_call(
        store_kernel,
        name="store",
        out_shape=jax.ShapeDtypeStruct(held.shape, BF16),
        in_specs=[vmem],
        out_specs=anywhere,
        scratch_shapes=[dma((FRAMES,))],
    )(pltpu.with_memory_space_constraint(held, pltpu.VMEM))


def solution(mesh):
    return jax.shard_map(
        on_device,
        mesh=mesh,
        in_specs=(P(("grp", "ha"), None), P("grp"), P("grp"), P(), P(), P(), P(), P(), P(), P()),
        out_specs=P(None, ("grp", "ha"), None, None),
        check_vma=False,
    )
```

```python
import functools

import jax
import jax.numpy as jnp
from jax import lax
from jax.experimental import pallas as pl
from jax.experimental.pallas import tpu as pltpu
from jax.sharding import PartitionSpec as P

FRAMES = 4
VMEM_BYTES = 56_000_000
GROUP = 2
TILE = 32
MESH = pl.DeviceIdType.MESH
F32, BF16 = jnp.float32, jnp.bfloat16


def iota(shape, dim):
    return lax.broadcasted_iota(jnp.int32, shape, dim)


def expansion(lch):
    wide = 4 * lch
    i = iota((2 * wide, 6 * 2 * wide), 0)
    o = iota((2 * wide, 6 * 2 * wide), 1)
    half, q, r, k = i // wide, i // (2 * lch) % 2, i // lch % 2, i % lch
    block, lane = o // (2 * wide), o % (2 * wide)
    ohalf, kind = block // 3, block % 3
    oq, j, ok = lane // wide, lane // lch % 4, lane % lch
    same = (half == ohalf) & (q == oq) & (k == ok)
    own = (kind == 0) & (j == r + 1)
    before = (kind == 1) & (r == 1) & (j == 0)
    after = (kind == 2) & (r == 0) & (j == 3)
    return jnp.where(same & (own | before | after), 1.0, 0.0).astype(BF16)


def kernel(
    n, lch, ch,
    tokens, shift_in, scale_in, hw, hbias_in, k1, b1_in, gain_in, k2, b2_in, obuf,
    tok, hwv, k1v, w1, w2, blank, send, recv, patches, hid, filters, fields, products, z, inter,
    shift, scale, hbias, b1, gain, b2,
    tok_sem, hw_sem, k1_sem, w2_sem, send_sem, recv_sem, small_sem,
):
    me = lax.axis_index("ha")
    per = n // FRAMES
    mine = lax.rem(me, per) * FRAMES
    frame = lax.div(me, per)
    cells = tok.shape[0] // FRAMES
    half = cells // 2
    width = tok.shape[1]
    wide = 4 * lch
    lanes = 2 * wide

    step = GROUP * cells
    steps = FRAMES // GROUP
    def token_copies(g):
        for i in range(g * GROUP, (g + 1) * GROUP):
            rows = pl.ds(i * cells, cells)
            yield pltpu.make_async_copy(tokens.at[rows], tok.at[rows], tok_sem.at[i])

    small = [
        pltpu.make_async_copy(src, dst, small_sem.at[i])
        for i, (src, dst) in enumerate(zip((scale_in, shift_in, hbias_in, b1_in, gain_in, b2_in), (scale, shift, hbias, b1, gain, b2)))
    ]
    for copy in token_copies(0):
        copy.start()
    for g in range(2):
        pltpu.make_async_copy(hw, hwv.at[pl.ds(g * wide, wide)], hw_sem.at[g]).start()
    for copy in small:
        copy.start()
    for g in range(1, steps):
        for copy in token_copies(g):
            copy.start()

    def kernel_copy(t):
        taps = pl.ds((8 - t) * 3, 3)
        return pltpu.make_async_copy(k2.at[taps], w2.at[taps], w2_sem.at[t])

    barrier = pltpu.get_barrier_semaphore()
    for f in range(FRAMES):
        for g in range(3):
            p = me + g - 1
            src = f * per + lax.div(jnp.clip(p, 0, n - 1), FRAMES)

            @pl.when((p >= 0) & (p < n) & (src != me))
            def _():
                pl.semaphore_signal(barrier, inc=1, device_id={"ha": src}, device_id_type=MESH)

    def targets(j):
        for g in range(3):
            to = mine + j + 1 - g
            yield g, to, (to >= 0) & (to < n)

    credits = 0
    for j in range(FRAMES):
        for g, to, ok in targets(j):
            credits = credits + jnp.where(ok & (to != me), 1, 0)

    w1[...] = jnp.zeros_like(w1)
    blank[...] = jnp.zeros_like(blank)
    for g in (0, 2):
        @pl.when(me == (0 if g == 0 else n - 1))
        def _():
            for f in range(FRAMES):
                pltpu.make_async_copy(blank, recv.at[f, g], recv_sem.at[f, g]).start()

    def head_rows(s):
        rows = pl.ds(s * step, step)
        acc = jnp.zeros((step, 128), F32)
        for c in range(0, width, 128):
            acc += tok[rows, c:c + 128].astype(F32)
        mean = jnp.sum(acc, axis=1, keepdims=True) * (1.0 / width)
        acc = jnp.zeros((step, 128), F32)
        for c in range(0, width, 128):
            centred = tok[rows, c:c + 128].astype(F32) - mean
            acc += centred * centred
        spread = jnp.sum(acc, axis=1, keepdims=True) * (1.0 / width)
        inv = lax.rsqrt(spread + 1e-06)
        if s == 0:
            for g in range(2):
                pltpu.make_async_copy(hw, hwv.at[pl.ds(g * wide, wide)], hw_sem.at[g]).wait()
            for copy in small:
                copy.wait()
        total = jnp.zeros((step, lanes), F32)
        for c in range(0, width, 512):
            centred = tok[rows, c:c + 512].astype(F32) - mean
            modulated = (centred * inv * scale[:, c:c + 512] + shift[:, c:c + 512]).astype(BF16)
            total += lax.dot_general(modulated, hwv[:, c:c + 512], (((1,), (1,)), ((), ())), preferred_element_type=F32)
        total = total + jnp.concatenate([hbias[...], hbias[...]], axis=1)
        low = iota((half, lanes), 1) < wide
        for a in range(GROUP):
            row = total[a * cells:(a + 1) * cells]
            send[s * GROUP + a] = jnp.where(low, row[:half], row[half:]).astype(BF16)

    for s in range(steps):
        for copy in token_copies(s):
            copy.wait()
        if s == 0:
            pltpu.make_async_copy(k1, k1v, k1_sem).start()
            for t in range(9):
                kernel_copy(t).start()
        head_rows(s)
        if s == 0:
            pl.semaphore_wait(barrier, credits)
        for a in range(GROUP):
            j = s * GROUP + a
            for g, to, ok in targets(j):
                @pl.when(ok & (to != me))
                def _():
                    pltpu.make_async_remote_copy(
                        src_ref=send.at[j], dst_ref=recv.at[frame, g],
                        send_sem=send_sem.at[j, g], recv_sem=recv_sem.at[frame, g],
                        device_id={"ha": to}, device_id_type=MESH,
                    ).start()

                @pl.when(ok & (to == me))
                def _():
                    pltpu.make_async_copy(send.at[j], recv.at[frame, g], recv_sem.at[frame, g]).start()

    pltpu.make_async_copy(k1, k1v, k1_sem).wait()
    tap = 3 * lch
    for dt in range(3):
        for s in range(2):
            for r in range(2):
                for dy in range(3):
                    top = dt * 2 * lanes + (dy + s) * wide + r * lch
                    w1[top:top + tap, (2 * s + r) * ch:(2 * s + r + 1) * ch] = k1v[(dt * 3 + dy) * tap:(dt * 3 + dy + 1) * tap, :]
    spread_lanes = expansion(lch)
    place = iota((cells, lanes), 0)
    bias1, gains = [jnp.concatenate([v[i:i + 1] for i in range(ch // 128)], axis=1) for v in (b1, gain)]
    gains = 0.5 * gains

    def both(a, b, c):
        ends = a + c
        return ends + b, ends - b

    def transform(dt, rows, into):
        raw = [[w2[dt * 9 + dy * 3 + dx, rows, :] for dx in range(3)] for dy in range(3)]
        taps = [[x.astype(F32) for x in line] for line in raw]
        for i in (0, 3):
            for j in (0, 3):
                filters[4 * i + j, into, :] = raw[2 * i // 3][2 * j // 3]
        for j in (0, 3):
            one, two = both(*[taps[dy][2 * j // 3] for dy in range(3)])
            filters[4 + j, into, :] = one.astype(BF16)
            filters[8 + j, into, :] = two.astype(BF16)
        lines = [both(*taps[dy]) for dy in range(3)]
        for j in (1, 2):
            for i in (0, 3):
                filters[4 * i + j, into, :] = lines[2 * i // 3][j - 1].astype(BF16)
            one, two = both(*[lines[dy][j - 1] for dy in range(3)])
            filters[4 + j, into, :] = one.astype(BF16)
            filters[8 + j, into, :] = two.astype(BF16)

    for dt in (2, 1, 0):
        for t in range(6 - 3 * dt, 9 - 3 * dt):
            kernel_copy(t).wait()

        def body(r, carry):
            transform(dt, pl.ds(pl.multiple_of(r * TILE, TILE), TILE), pl.ds(pl.multiple_of(dt * ch + r * TILE, TILE), TILE))
            return carry

        lax.fori_loop(0, ch // TILE, body, 0)
    edge = iota((cells, 128), 0)

    def arrive(pair):
        for f in (2 * pair, 2 * pair + 1):
            for g in range(3):
                pltpu.make_async_copy(blank, recv.at[f, g], recv_sem.at[f, g]).wait()

    def hidden_pair(pair):
        frames = (2 * pair, 2 * pair + 1)
        rows = jnp.concatenate([recv[f].reshape(3 * half, lanes) for f in frames], axis=0)
        opened = jnp.dot(rows, spread_lanes, preferred_element_type=F32)
        for at, f in enumerate(frames):
            for g in range(3):
                got = opened[(3 * at + g) * half:(3 * at + g + 1) * half]
                own, before, after = [
                    jnp.concatenate([got[:, kind * lanes:(kind + 1) * lanes], got[:, (3 + kind) * lanes:(4 + kind) * lanes]], axis=0)
                    for kind in range(3)
                ]
                before = jnp.where(place == 0, 0.0, pltpu.roll(before, 1, 0))
                after = jnp.where(place == cells - 1, 0.0, pltpu.roll(after, cells - 1, 0))
                patches[f, :, g * lanes:(g + 1) * lanes] = (own + before + after).astype(BF16)

        first_dt = max(0, 1 - 2 * pair)
        empty = jnp.zeros((cells, 2 * lanes), BF16)
        left = jnp.concatenate([
            jnp.concatenate(
                [patches[f + dt - 2, :, p * lanes:(p + 2) * lanes] if f + dt >= 2 else empty for dt in range(first_dt, 3)], axis=1)
            for f in frames for p in range(2)], axis=0)
        for s in range(2):
            first = jnp.dot(left, w1[first_dt * 2 * lanes:, 2 * s * ch:2 * (s + 1) * ch], preferred_element_type=F32)
            for at, f in enumerate(frames):
                for p in range(2):
                    y = 2 * p + s
                    top = (2 * at + p) * cells
                    for r in range(2):
                        v = first[top:top + cells, r * ch:(r + 1) * ch] + bias1
                        meansq = jnp.sum(v * v, axis=1, keepdims=True) * (1.0 / ch)
                        inv = lax.rsqrt(meansq + 1e-06)
                        if y == 0:
                            inv = jnp.where(me == 0, 0.0, inv)
                        if y == 3:
                            inv = jnp.where(me == n - 1, 0.0, inv)
                        v = v * inv * gains
                        v = v * jnp.tanh(v) + v
                        hid[f, y, r] = v.astype(BF16)
        for f in frames:
            for c in range(0, ch, 128):
                def row(y, r):
                    return hid[f, y, r, :, c:c + 128].astype(F32)

                for i, (one, two) in enumerate(((0, 2), (1, 2), (2, 1), (1, 3))):
                    even, odd = [row(one, r) + row(two, r) if i == 1 else row(one, r) - row(two, r) for r in range(2)]
                    ahead = jnp.where(edge == 0, 0.0, pltpu.roll(odd, 1, 0))
                    behind = jnp.where(edge == cells - 1, 0.0, pltpu.roll(even, cells - 1, 0))
                    for j, value in enumerate((ahead - odd, even + odd, odd - even, even - behind)):
                        fields[4 * i + j, f, :, c:c + 128] = value.astype(BF16)

    def decoded_pair(pair):
        frames = (2 * pair, 2 * pair + 1)
        first_dt = max(0, 1 - 2 * pair)
        empty = jnp.zeros((cells, ch), BF16)
        for j in range(4):
            for i in range(4):
                k = 4 * i + j
                left = jnp.concatenate([
                    jnp.concatenate([fields[k, f + dt - 2] if f + dt >= 2 else empty for dt in range(first_dt, 3)], axis=1)
                    for f in frames], axis=0)
                products[j % 2, i] = jnp.dot(left, filters[k, first_dt * ch:, :], preferred_element_type=F32)
            u = [products[j % 2, i] for i in range(4)]
            for y, value in enumerate((u[0] + 0.5 * (u[1] + u[2]), 0.5 * (u[1] - u[2]) - u[3])):
                if j in (1, 2):
                    value = 0.5 * value
                if j == 0:
                    z[pair, y, 0] = value
                if j == 1:
                    z[pair, y, 0] += value
                    z[pair, y, 1] = value
                if j == 2:
                    z[pair, y, 0] += value
                    z[pair, y, 1] -= value
                if j == 3:
                    z[pair, y, 1] -= value
        for at, f in enumerate(frames):
            top = at * cells
            for y in range(2):
                for c in range(0, ch, 128):
                    bias = b2[c // 128:c // 128 + 1]
                    lane = inter.at[f, y, c // 128]
                    for r in range(2):
                        lane[pl.ds(r, cells, stride=2), :] = z[pair, y, r, top:top + cells, c:c + 128] + bias
                    obuf[f, y, :, c:c + 128] = lane[...].astype(BF16)

    for pair in range(FRAMES // 2):
        arrive(pair)
        hidden_pair(pair)
        decoded_pair(pair)

    for j in range(FRAMES):
        for g, to, ok in targets(j):
            @pl.when(ok & (to != me))
            def _():
                pltpu.make_async_remote_copy(
                    src_ref=send.at[j], dst_ref=recv.at[frame, g],
                    send_sem=send_sem.at[j, g], recv_sem=recv_sem.at[frame, g],
                    device_id={"ha": to}, device_id_type=MESH,
                ).wait_send()


def store_kernel(held, out, sem):
    copies = [pltpu.make_async_copy(held.at[f], out.at[f], sem.at[f]) for f in range(FRAMES)]
    for copy in copies:
        copy.start()
    for copy in copies:
        copy.wait()


def on_device(tokens, mod_shift, mod_scale, head_weight, head_bias, first_kernel, first_bias, norm_gain, second_kernel, second_bias):
    n = lax.axis_size("ha")
    count, width = tokens.shape
    lch, ch = first_kernel.shape[3:]
    cells = count // FRAMES
    lanes = 8 * lch
    anywhere = pl.BlockSpec(memory_space=pl.ANY)
    vmem = pl.BlockSpec(memory_space=pltpu.VMEM)
    dma = pltpu.SemaphoreType.DMA
    held = pl.pallas_call(
        functools.partial(kernel, n, lch, ch),
        name="decode",
        out_shape=pltpu.VMEM((FRAMES, 2, 2 * cells, ch), BF16),
        in_specs=[anywhere] * 10,
        out_specs=vmem,
        scratch_shapes=[
            pltpu.VMEM((count, width), BF16),
            pltpu.VMEM((lanes, width), BF16),
            pltpu.VMEM((27 * lch, ch), BF16),
            pltpu.VMEM((6 * lanes, 4 * ch), BF16),
            pltpu.VMEM((27, ch, ch), BF16),
            pltpu.VMEM((cells // 2, lanes), BF16),
            pltpu.VMEM((FRAMES, cells // 2, lanes), BF16),
            pltpu.VMEM((FRAMES, 3, cells // 2, lanes), BF16),
            pltpu.VMEM((FRAMES, cells, 3 * lanes), BF16),
            pltpu.VMEM((FRAMES, 4, 2, cells, ch), BF16),
            pltpu.VMEM((16, 3 * ch, ch), BF16),
            pltpu.VMEM((16, FRAMES, cells, ch), BF16),
            pltpu.VMEM((2, 4, 2 * cells, ch), F32),
            pltpu.VMEM((FRAMES // 2, 2, 2, 2 * cells, ch), F32),
            pltpu.VMEM((FRAMES, 2, ch // 128, 2 * cells, 128), F32),
            pltpu.VMEM((1, width), F32),
            pltpu.VMEM((1, width), F32),
            pltpu.VMEM((1, 4 * lch), F32),
            pltpu.VMEM((ch // 128, 128), F32),
            pltpu.VMEM((ch // 128, 128), F32),
            pltpu.VMEM((ch // 128, 128), F32),
            dma((FRAMES,)),
            dma((2,)),
            dma,
            dma((9,)),
            dma((FRAMES, 3)),
            dma((FRAMES, 3)),
            dma((6,)),
        ],
        compiler_params=pltpu.CompilerParams(collective_id=0, has_side_effects=True, vmem_limit_bytes=VMEM_BYTES),
    )(
        tokens, mod_shift.reshape(1, width), mod_scale.reshape(1, width), head_weight.T, head_bias.reshape(1, -1),
        first_kernel.reshape(27 * lch, ch), first_bias.reshape(-1, 128), norm_gain.reshape(-1, 128),
        second_kernel.reshape(27, ch, ch), second_bias.reshape(-1, 128),
    )
    return pl.pallas_call(
        store_kernel,
        name="store",
        out_shape=jax.ShapeDtypeStruct(held.shape, BF16),
        in_specs=[vmem],
        out_specs=anywhere,
        scratch_shapes=[dma((FRAMES,))],
    )(pltpu.with_memory_space_constraint(held, pltpu.VMEM))


def solution(mesh):
    return jax.shard_map(
        on_device,
        mesh=mesh,
        in_specs=(P(("grp", "ha"), None), P("grp"), P("grp"), P(), P(), P(), P(), P(), P(), P()),
        out_specs=P(None, ("grp", "ha"), None, None),
        check_vma=False,
    )
```

```python
import functools

import jax
import jax.numpy as jnp
from jax import lax
from jax.experimental import pallas as pl
from jax.experimental.pallas import tpu as pltpu
from jax.sharding import PartitionSpec as P

FRAMES = 4
VMEM_BYTES = 56_000_000
GROUP = 2
TILE = 32
DIRECT = 2
MESH = pl.DeviceIdType.MESH
F32, BF16 = jnp.float32, jnp.bfloat16


def iota(shape, dim):
    return lax.broadcasted_iota(jnp.int32, shape, dim)


def expansion(lch):
    wide = 4 * lch
    i = iota((2 * wide, 6 * 2 * wide), 0)
    o = iota((2 * wide, 6 * 2 * wide), 1)
    half, q, r, k = i // wide, i // (2 * lch) % 2, i // lch % 2, i % lch
    block, lane = o // (2 * wide), o % (2 * wide)
    ohalf, kind = block // 3, block % 3
    oq, j, ok = lane // wide, lane // lch % 4, lane % lch
    same = (half == ohalf) & (q == oq) & (k == ok)
    own = (kind == 0) & (j == r + 1)
    before = (kind == 1) & (r == 1) & (j == 0)
    after = (kind == 2) & (r == 0) & (j == 3)
    return jnp.where(same & (own | before | after), 1.0, 0.0).astype(BF16)


def kernel(
    n, lch, ch,
    tokens, shift_in, scale_in, hw, hbias_in, k1, b1_in, gain_in, k2, b2_in, obuf,
    tok, offsets, hwv, k1v, w1, w2, blank, send, recv, patches, hid, filters, fields, products, z, inter,
    shift, scale, hbias, b1, gain, b2,
    tok_sem, hw_sem, k1_sem, w2_sem, send_sem, recv_sem, small_sem, swap_sem,
):
    me = lax.axis_index("ha")
    per = n // FRAMES
    mine = lax.rem(me, per) * FRAMES
    frame = lax.div(me, per)
    cells = tok.shape[0] // FRAMES
    half = cells // 2
    width = tok.shape[1]
    wide = 4 * lch
    lanes = 2 * wide

    step = GROUP * cells
    steps = FRAMES // GROUP
    def token_copies(g):
        for i in range(g * GROUP, (g + 1) * GROUP):
            rows = pl.ds(i * cells, cells)
            yield pltpu.make_async_copy(tokens.at[rows], tok.at[rows], tok_sem.at[i])

    small = [
        pltpu.make_async_copy(src, dst, small_sem.at[i])
        for i, (src, dst) in enumerate(zip((scale_in, shift_in, hbias_in, b1_in, gain_in, b2_in), (scale, shift, hbias, b1, gain, b2)))
    ]
    for copy in token_copies(0):
        copy.start()
    for g in range(2):
        pltpu.make_async_copy(hw, hwv.at[pl.ds(g * wide, wide)], hw_sem.at[g]).start()
    for copy in small:
        copy.start()
    for g in range(1, steps):
        for copy in token_copies(g):
            copy.start()

    def kernel_copy(t):
        taps = pl.ds((8 - t) * 3, 3)
        return pltpu.make_async_copy(k2.at[taps], w2.at[taps], w2_sem.at[t])

    barrier = pltpu.get_barrier_semaphore()
    twin = me + 1 - 2 * lax.rem(me, 2)
    across = 2 * lax.rem(me, 2)
    pl.semaphore_signal(barrier, inc=1, device_id={"ha": twin}, device_id_type=MESH)
    for f in range(FRAMES):
        for p in (me, me - 1 + across) + ((twin,) if f >= DIRECT else ()):
            src = f * per + lax.div(jnp.clip(p, 0, n - 1), FRAMES)

            @pl.when((p >= 0) & (p < n) & (src != me))
            def _():
                pl.semaphore_signal(barrier, inc=1, device_id={"ha": src}, device_id_type=MESH)

    def targets(j):
        for g in (1, 2 if j % 2 == 0 else 0):
            to = mine + j + 1 - g
            yield g, to, (to >= 0) & (to < n)
        g = 0 if j % 2 == 0 else 2
        yield g, mine + j + 1 - g, frame >= DIRECT

    def swap(f):
        return pltpu.make_async_remote_copy(
            src_ref=recv.at[f, 1], dst_ref=recv.at[f, across],
            send_sem=swap_sem.at[f], recv_sem=recv_sem.at[f, across],
            device_id={"ha": twin}, device_id_type=MESH,
        )

    def forward(frames):
        for f in frames:
            pltpu.make_async_copy(blank, recv.at[f, 1], recv_sem.at[f, 1]).wait()
            swap(f).start()

    credits = 1
    for j in range(FRAMES):
        for g, to, ok in targets(j):
            credits = credits + jnp.where(ok & (to != me), 1, 0)

    w1[...] = jnp.zeros_like(w1)
    blank[...] = jnp.zeros_like(blank)
    for g in (0, 2):
        @pl.when(me == (0 if g == 0 else n - 1))
        def _():
            for f in range(FRAMES):
                pltpu.make_async_copy(blank, recv.at[f, g], recv_sem.at[f, g]).start()

    def head_rows(s):
        rows = pl.ds(s * step, step)
        acc = jnp.zeros((step, 128), F32)
        for c in range(0, width, 128):
            acc += tok[rows, c:c + 128].astype(F32)
        mean = jnp.sum(acc, axis=1, keepdims=True) * (1.0 / width)
        acc = jnp.zeros((step, 128), F32)
        for c in range(0, width, 128):
            centred = tok[rows, c:c + 128].astype(F32) - mean
            offsets[:, c:c + 128] = centred
            acc += centred * centred
        spread = jnp.sum(acc, axis=1, keepdims=True) * (1.0 / width)
        inv = lax.rsqrt(spread + 1e-06)
        if s == 0:
            for g in range(2):
                pltpu.make_async_copy(hw, hwv.at[pl.ds(g * wide, wide)], hw_sem.at[g]).wait()
            for copy in small:
                copy.wait()
        total = jnp.zeros((step, lanes), F32)
        for c in range(0, width, 512):
            modulated = (offsets[:, c:c + 512] * inv * scale[:, c:c + 512] + shift[:, c:c + 512]).astype(BF16)
            total += lax.dot_general(modulated, hwv[:, c:c + 512], (((1,), (1,)), ((), ())), preferred_element_type=F32)
        total = total + jnp.concatenate([hbias[...], hbias[...]], axis=1)
        low = iota((half, lanes), 1) < wide
        for a in range(GROUP):
            row = total[a * cells:(a + 1) * cells]
            send[s * GROUP + a] = jnp.where(low, row[:half], row[half:]).astype(BF16)

    for s in range(steps):
        for copy in token_copies(s):
            copy.wait()
        if s == 0:
            pltpu.make_async_copy(k1, k1v, k1_sem).start()
            for t in range(9):
                kernel_copy(t).start()
        head_rows(s)
        if s == 0:
            pl.semaphore_wait(barrier, credits)
        for k in range(3 * GROUP):
            j = s * GROUP + k % GROUP
            for g, to, ok in list(targets(j))[k // GROUP:k // GROUP + 1]:
                @pl.when(ok & (to != me))
                def _():
                    pltpu.make_async_remote_copy(
                        src_ref=send.at[j], dst_ref=recv.at[frame, g],
                        send_sem=send_sem.at[j, g], recv_sem=recv_sem.at[frame, g],
                        device_id={"ha": to}, device_id_type=MESH,
                    ).start()

                @pl.when(ok & (to == me))
                def _():
                    pltpu.make_async_copy(send.at[j], recv.at[frame, g], recv_sem.at[frame, g]).start()

    pltpu.make_async_copy(k1, k1v, k1_sem).wait()
    tap = 3 * lch
    for dt in range(3):
        for s in range(2):
            for r in range(2):
                for dy in range(3):
                    top = dt * 2 * lanes + (dy + s) * wide + r * lch
                    w1[top:top + tap, (2 * s + r) * ch:(2 * s + r + 1) * ch] = k1v[(dt * 3 + dy) * tap:(dt * 3 + dy + 1) * tap, :]
    spread_lanes = expansion(lch)
    place = iota((cells, lanes), 0)
    bias1, gains = [jnp.concatenate([v[i:i + 1] for i in range(ch // 128)], axis=1) for v in (b1, gain)]
    gains = 0.5 * gains

    def both(a, b, c):
        ends = a + c
        return ends + b, ends - b

    def transform(dt, rows, into):
        raw = [[w2[dt * 9 + dy * 3 + dx, rows, :] for dx in range(3)] for dy in range(3)]
        taps = [[x.astype(F32) for x in line] for line in raw]
        for i in (0, 3):
            for j in (0, 3):
                filters[4 * i + j, into, :] = raw[2 * i // 3][2 * j // 3]
        for j in (0, 3):
            one, two = both(*[taps[dy][2 * j // 3] for dy in range(3)])
            filters[4 + j, into, :] = one.astype(BF16)
            filters[8 + j, into, :] = two.astype(BF16)
        lines = [both(*taps[dy]) for dy in range(3)]
        for j in (1, 2):
            for i in (0, 3):
                filters[4 * i + j, into, :] = lines[2 * i // 3][j - 1].astype(BF16)
            one, two = both(*[lines[dy][j - 1] for dy in range(3)])
            filters[4 + j, into, :] = one.astype(BF16)
            filters[8 + j, into, :] = two.astype(BF16)

    for dt in (2, 1, 0):
        if dt == 0:
            forward((0, 1))
        for t in range(6 - 3 * dt, 9 - 3 * dt):
            kernel_copy(t).wait()

        def body(r, carry):
            transform(dt, pl.ds(pl.multiple_of(r * TILE, TILE), TILE), pl.ds(pl.multiple_of(dt * ch + r * TILE, TILE), TILE))
            return carry

        lax.fori_loop(0, ch // TILE, body, 0)
    edge = iota((cells, 128), 0)

    def arrive(pair):
        for f in (2 * pair, 2 * pair + 1):
            for g in (0, 2) if f < DIRECT else range(3):
                pltpu.make_async_copy(blank, recv.at[f, g], recv_sem.at[f, g]).wait()

    def hidden_pair(pair):
        frames = (2 * pair, 2 * pair + 1)
        rows = jnp.concatenate([recv[f].reshape(3 * half, lanes) for f in frames], axis=0)
        opened = jnp.dot(rows, spread_lanes, preferred_element_type=F32)
        for at, f in enumerate(frames):
            for g in range(3):
                got = opened[(3 * at + g) * half:(3 * at + g + 1) * half]
                own, before, after = [
                    jnp.concatenate([got[:, kind * lanes:(kind + 1) * lanes], got[:, (3 + kind) * lanes:(4 + kind) * lanes]], axis=0)
                    for kind in range(3)
                ]
                before = jnp.where(place == 0, 0.0, pltpu.roll(before, 1, 0))
                after = jnp.where(place == cells - 1, 0.0, pltpu.roll(after, cells - 1, 0))
                patches[f, :, g * lanes:(g + 1) * lanes] = (own + before + after).astype(BF16)

        first_dt = max(0, 1 - 2 * pair)
        empty = jnp.zeros((cells, 2 * lanes), BF16)
        left = jnp.concatenate([
            jnp.concatenate(
                [patches[f + dt - 2, :, p * lanes:(p + 2) * lanes] if f + dt >= 2 else empty for dt in range(first_dt, 3)], axis=1)
            for f in frames for p in range(2)], axis=0)
        for s in range(2):
            first = jnp.dot(left, w1[first_dt * 2 * lanes:, 2 * s * ch:2 * (s + 1) * ch], preferred_element_type=F32)
            for at, f in enumerate(frames):
                for p in range(2):
                    y = 2 * p + s
                    top = (2 * at + p) * cells
                    for r in range(2):
                        v = first[top:top + cells, r * ch:(r + 1) * ch] + bias1
                        meansq = jnp.sum(v * v, axis=1, keepdims=True) * (1.0 / ch)
                        inv = lax.rsqrt(meansq + 1e-06)
                        if y == 0:
                            inv = jnp.where(me == 0, 0.0, inv)
                        if y == 3:
                            inv = jnp.where(me == n - 1, 0.0, inv)
                        v = v * inv * gains
                        v = v * jnp.tanh(v) + v
                        hid[f, y, r] = v.astype(BF16)
        for f in frames:
            for c in range(0, ch, 128):
                def row(y, r):
                    return hid[f, y, r, :, c:c + 128].astype(F32)

                for i, (one, two) in enumerate(((0, 2), (1, 2), (2, 1), (1, 3))):
                    even, odd = [row(one, r) + row(two, r) if i == 1 else row(one, r) - row(two, r) for r in range(2)]
                    ahead = jnp.where(edge == 0, 0.0, pltpu.roll(odd, 1, 0))
                    behind = jnp.where(edge == cells - 1, 0.0, pltpu.roll(even, cells - 1, 0))
                    for j, value in enumerate((ahead - odd, even + odd, odd - even, even - behind)):
                        fields[4 * i + j, f, :, c:c + 128] = value.astype(BF16)

    def decoded_pair(pair):
        frames = (2 * pair, 2 * pair + 1)
        first_dt = max(0, 1 - 2 * pair)
        empty = jnp.zeros((cells, ch), BF16)
        for j in range(4):
            for i in range(4):
                k = 4 * i + j
                left = jnp.concatenate([
                    jnp.concatenate([fields[k, f + dt - 2] if f + dt >= 2 else empty for dt in range(first_dt, 3)], axis=1)
                    for f in frames], axis=0)
                products[j % 2, i] = jnp.dot(left, filters[k, first_dt * ch:, :], preferred_element_type=F32)
            u = [products[j % 2, i] for i in range(4)]
            for y, value in enumerate((u[0] + 0.5 * (u[1] + u[2]), 0.5 * (u[1] - u[2]) - u[3])):
                if j in (1, 2):
                    value = 0.5 * value
                if j == 0:
                    z[pair, y, 0] = value
                if j == 1:
                    z[pair, y, 0] += value
                    z[pair, y, 1] = value
                if j == 2:
                    z[pair, y, 0] += value
                    z[pair, y, 1] -= value
                if j == 3:
                    z[pair, y, 1] -= value
        for at, f in enumerate(frames):
            top = at * cells
            for y in range(2):
                for c in range(0, ch, 128):
                    bias = b2[c // 128:c // 128 + 1]
                    lane = inter.at[f, y, c // 128]
                    for r in range(2):
                        lane[pl.ds(r, cells, stride=2), :] = z[pair, y, r, top:top + cells, c:c + 128] + bias
                    obuf[f, y, :, c:c + 128] = lane[...].astype(BF16)

    for pair in range(FRAMES // 2):
        arrive(pair)
        hidden_pair(pair)
        decoded_pair(pair)

    for j in range(FRAMES):
        for g, to, ok in targets(j):
            @pl.when(ok & (to != me))
            def _():
                pltpu.make_async_remote_copy(
                    src_ref=send.at[j], dst_ref=recv.at[frame, g],
                    send_sem=send_sem.at[j, g], recv_sem=recv_sem.at[frame, g],
                    device_id={"ha": to}, device_id_type=MESH,
                ).wait_send()
    for f in range(DIRECT):
        swap(f).wait_send()


def store_kernel(held, out, sem):
    copies = [pltpu.make_async_copy(held.at[f], out.at[f], sem.at[f]) for f in range(FRAMES)]
    for copy in copies:
        copy.start()
    for copy in copies:
        copy.wait()


def on_device(tokens, mod_shift, mod_scale, head_weight, head_bias, first_kernel, first_bias, norm_gain, second_kernel, second_bias):
    n = lax.axis_size("ha")
    count, width = tokens.shape
    lch, ch = first_kernel.shape[3:]
    cells = count // FRAMES
    lanes = 8 * lch
    anywhere = pl.BlockSpec(memory_space=pl.ANY)
    vmem = pl.BlockSpec(memory_space=pltpu.VMEM)
    dma = pltpu.SemaphoreType.DMA
    held = pl.pallas_call(
        functools.partial(kernel, n, lch, ch),
        name="decode",
        out_shape=pltpu.VMEM((FRAMES, 2, 2 * cells, ch), BF16),
        in_specs=[anywhere] * 10,
        out_specs=vmem,
        scratch_shapes=[
            pltpu.VMEM((count, width), BF16),
            pltpu.VMEM((GROUP * cells, width), F32),
            pltpu.VMEM((lanes, width), BF16),
            pltpu.VMEM((27 * lch, ch), BF16),
            pltpu.VMEM((6 * lanes, 4 * ch), BF16),
            pltpu.VMEM((27, ch, ch), BF16),
            pltpu.VMEM((cells // 2, lanes), BF16),
            pltpu.VMEM((FRAMES, cells // 2, lanes), BF16),
            pltpu.VMEM((FRAMES, 3, cells // 2, lanes), BF16),
            pltpu.VMEM((FRAMES, cells, 3 * lanes), BF16),
            pltpu.VMEM((FRAMES, 4, 2, cells, ch), BF16),
            pltpu.VMEM((16, 3 * ch, ch), BF16),
            pltpu.VMEM((16, FRAMES, cells, ch), BF16),
            pltpu.VMEM((2, 4, 2 * cells, ch), F32),
            pltpu.VMEM((FRAMES // 2, 2, 2, 2 * cells, ch), F32),
            pltpu.VMEM((FRAMES, 2, ch // 128, 2 * cells, 128), F32),
            pltpu.VMEM((1, width), F32),
            pltpu.VMEM((1, width), F32),
            pltpu.VMEM((1, 4 * lch), F32),
            pltpu.VMEM((ch // 128, 128), F32),
            pltpu.VMEM((ch // 128, 128), F32),
            pltpu.VMEM((ch // 128, 128), F32),
            dma((FRAMES,)),
            dma((2,)),
            dma,
            dma((9,)),
            dma((FRAMES, 3)),
            dma((FRAMES, 3)),
            dma((6,)),
            dma((DIRECT,)),
        ],
        compiler_params=pltpu.CompilerParams(collective_id=0, has_side_effects=True, vmem_limit_bytes=VMEM_BYTES),
    )(
        tokens, mod_shift.reshape(1, width), mod_scale.reshape(1, width), head_weight.T, head_bias.reshape(1, -1),
        first_kernel.reshape(27 * lch, ch), first_bias.reshape(-1, 128), norm_gain.reshape(-1, 128),
        second_kernel.reshape(27, ch, ch), second_bias.reshape(-1, 128),
    )
    return pl.pallas_call(
        store_kernel,
        name="store",
        out_shape=jax.ShapeDtypeStruct(held.shape, BF16),
        in_specs=[vmem],
        out_specs=anywhere,
        scratch_shapes=[dma((FRAMES,))],
    )(pltpu.with_memory_space_constraint(held, pltpu.VMEM))


def solution(mesh):
    return jax.shard_map(
        on_device,
        mesh=mesh,
        in_specs=(P(("grp", "ha"), None), P("grp"), P("grp"), P(), P(), P(), P(), P(), P(), P()),
        out_specs=P(None, ("grp", "ha"), None, None),
        check_vma=False,
    )
```
